32 devices in a mesh: fluid: 8 (over y, x, core), solid: 4 (over z).
Axes of the slice: x: 2, y: 2, z: 4, core: 2. Of those that a mesh axis runs over, the one named last changes fastest.
Arguments:
- earlier_thermal_state: float32 [256, 128, 128], P('fluid', 'solid'), may hold values from -6 to 6
- thermal_inertia: float32 [256, 128, 128], P('fluid', 'solid'), may hold values from 0.3 to 3
- boundary_energy_current: float32 [64, 16384], P(None, ('fluid', 'solid')), may hold values from -6 to 6
- jacobian_quad_factors: float32 [64, 32768], P(None, ('fluid', 'solid')), may hold values from 0.05 to 0.4
- patch_holder_liquid: int32 [32768, 1], P(('fluid', 'solid')), may hold values from 0 to 7; in each aligned block of 1024 rows (0 to 1023, 1024 to 2047, ...) at most 512 rows name the same one
- patch_slot_number: int32 [32768], P(('fluid', 'solid')), may hold values from 0 to 511
Outputs:
- thermal_state_guess: float32 [256, 128, 128], P('fluid', 'solid')
- equation_misfit: float32 [256, 128, 128], P('fluid', 'solid')
The draws below stay inside these ranges and needn't reach their ends.
Inputs may be any that keep to these rules, and one draw needn't show every extreme that they name: `patch_holder_liquid`: within the rows of one device, no owner index is named by more than 512 rows; in the rows of some device one owner index is named by exactly 512 rows.
All inputs are finite; a program needn't handle non-finite values.
Results may differ from the reference program's by a relative error of at most 0.00025.
Values sent between devices are 32-bit elements; how exact they have to be, the bound alone decides.
A program may use at most 64 MiB of HBM per device.

```python
import math
import jax
import jax.numpy as jnp
import numpy as np

CX = 32
CY = 32
FACE_DEV = 512
Q = 64
ITERS = 3
ICELLS = 1024
MOST = 512
SOLID_COUNT_X = 256
SOLID_COUNT_Y = 128
SOLID_COUNT_Z = 128
ROWS = 32768
FACES = 16384
N_FLUID = 8
N_SOLID = 4


def touch_ends(drawn, rng, smallest, high):
    spot = [jax.random.randint(jax.random.fold_in(rng, axis), (), 0, length) for axis, length in enumerate(drawn.shape)]
    main_axis = drawn.shape.index(max(drawn.shape))
    next_to = spot[:main_axis] + [(spot[main_axis] + 1) % drawn.shape[main_axis]] + spot[main_axis + 1:]
    return drawn.at[tuple(spot)].set(smallest).at[tuple(next_to)].set(high)


def level_of(own_key, shape, cuts, low, top_value):
    def one(axis_at, parts):
        heights = jax.random.uniform(jax.random.fold_in(jax.random.fold_in(own_key, 6), axis_at), (parts,), jnp.float32, low / len(cuts), top_value / len(cuts))
        return jnp.repeat(jnp.exp(heights), shape[axis_at] // parts).reshape((-1,) + (1,) * (len(shape) - axis_at - 1))

    factor_of = one(*cuts[0])
    for cut in cuts[1:]:
        factor_of = factor_of * one(*cut)
    return factor_of


def assign_block(own_key, own, number, rows, count, top, reach, lean):
    order = jax.random.permutation(own_key, count)
    packed, usual = portions_of(count, rows * top, reach, lean, True), portions_of(count, rows * top, reach, lean, False)
    places = jnp.arange(count)

    def named(sizes, turn):
        used = int((sizes > 0).sum())
        fixed = max(1, used // 4)
        passed = fixed + (places - fixed + turn * (used - fixed)) % max(1, count - fixed)
        return jnp.zeros((count,), jnp.int32).at[order[jnp.where(places < fixed, places, passed)]].set(jnp.asarray(sizes, jnp.int32))

    sizes = jnp.where(number % 4 == 0, named(packed, number // 4), named(usual, number - number // 4 - 1))
    mixed = jax.random.permutation(jax.random.fold_in(own, 3), count)
    donor, receiver = mixed[0:count // 2 * 2:2], mixed[1:count // 2 * 2:2]
    margin = jnp.minimum(sizes[donor] - 1, reach - sizes[receiver]) // 2
    margin = jnp.where((donor == order[0]) | (receiver == order[0]) | (sizes[receiver] == 0), 0, jnp.maximum(margin, 0))
    passed = jax.random.randint(jax.random.fold_in(own, 4), (count // 2,), 0, 1 << 20) % (margin + 1)
    sizes = sizes.at[donor].add(-passed).at[receiver].add(passed)
    items = jnp.searchsorted(jnp.cumsum(sizes), jnp.arange(rows * top), side="right").astype(jnp.int32)
    grid = items.reshape(top, rows).T
    grid = grid[jax.random.permutation(jax.random.fold_in(own, 1), rows)]
    turn = jax.random.randint(jax.random.fold_in(own, 2), (rows, 1), 0, top)
    return jnp.take_along_axis(grid, (jnp.arange(top)[None, :] + turn) % top, axis=1)


def portions_of(amount, total, bound, slope, full):
    weights = [(1 << 20) // math.isqrt(standing ** slope) + 1 for standing in range(1, amount + 1)]
    largest = bound if full else min(bound, max(-(-total // amount), total * weights[0] // sum(weights)))
    least = 1 if total - largest >= amount - 1 else 0
    given, rest = [largest] + [least] * (amount - 1), total - largest - least * (amount - 1)
    while rest > 0:
        free = [i for i in range(1, amount) if given[i] < largest] or [i for i in range(1, amount) if given[i] < bound]
        pool, left = sum([weights[i] for i in free]), rest
        for i in free:
            more = min(bound - given[i], max(1, left * weights[i] // pool), rest)
            given[i] = given[i] + more
            rest = rest - more
    return np.array(given)


def scatter_about(own_key, shape, spread, reach, cuts=(), kind=jnp.bfloat16):
    result = jax.random.normal(own_key, shape, jnp.float32) * spread
    if len(cuts) > 0:
        result = level_of(own_key, shape, cuts, -0.22, 0.18) * result
    return jnp.clip(result, min=-reach, max=reach).astype(kind)


def setup_inputs(seed: int = 0) -> dict:
    key_list = jax.random.split(jax.random.key(seed), 7)
    earlier_thermal_state = scatter_about(key_list[0], (SOLID_COUNT_X, SOLID_COUNT_Y, SOLID_COUNT_Z), 1.0, 6.0, ((0, 8), (1, 4)), jnp.float32)
    thermal_inertia = jnp.clip(jnp.exp(math.log(3.0) - 2.3025851 * jax.random.uniform(key_list[1], (SOLID_COUNT_X, SOLID_COUNT_Y, SOLID_COUNT_Z), jnp.float32) ** level_of(key_list[1], (SOLID_COUNT_X, SOLID_COUNT_Y, SOLID_COUNT_Z), ((0, 8), (1, 4)), -0.2, 0.2)), 0.3, 3.0)
    boundary_energy_current = scatter_about(key_list[2], (Q, FACES), 1.0, 6.0, ((1, 32),), jnp.float32)
    jacobian_quad_factors = jnp.clip(jnp.exp(math.log(0.4) - 2.0794415 * jax.random.uniform(key_list[3], (Q, ROWS), jnp.float32) ** level_of(key_list[3], (Q, ROWS), ((1, 32),), -0.2, 0.2)), 0.05, 0.4)
    patch_holder_liquid_keys = jax.random.split(jax.random.fold_in(key_list[4], 1), ROWS // ICELLS)
    patch_holder_liquid_turns = jax.random.permutation(jax.random.fold_in(key_list[4], 3), ROWS // ICELLS)
    patch_holder_liquid = jax.vmap(lambda own, number: assign_block(jax.random.fold_in(key_list[4], 2), own, number, ICELLS, N_FLUID, 1, MOST, 2))(patch_holder_liquid_keys, patch_holder_liquid_turns).reshape((ROWS, 1))
    patch_slot_number = touch_ends(jax.random.randint(key_list[5], (ROWS,), 0, FACE_DEV), jax.random.fold_in(key_list[5], 1), 0, FACE_DEV - 1).astype(jnp.int32)
    return {"earlier_thermal_state": earlier_thermal_state, "thermal_inertia": thermal_inertia, "boundary_energy_current": boundary_energy_current, "jacobian_quad_factors": jacobian_quad_factors, "patch_holder_liquid": patch_holder_liquid, "patch_slot_number": patch_slot_number}


def matrix_action(field, thermal_inertia):
    padded = jnp.pad(field, 1)
    beside = padded[2:, 1:-1, 1:-1] + padded[:-2, 1:-1, 1:-1]
    beside = beside + padded[1:-1, 2:, 1:-1] + padded[1:-1, :-2, 1:-1]
    beside = beside + padded[1:-1, 1:-1, 2:] + padded[1:-1, 1:-1, :-2]
    return (6.0 + thermal_inertia) * field - beside


def reference(earlier_thermal_state, thermal_inertia, boundary_energy_current, jacobian_quad_factors, patch_holder_liquid, patch_slot_number):
    icells = CX * CY
    rows_index = jnp.arange(ROWS, dtype=jnp.int32)
    device = rows_index // icells
    solid_index = device % N_SOLID
    owner_device = patch_holder_liquid[:, 0].astype(jnp.int32) * N_SOLID + solid_index
    columns = owner_device * FACE_DEV + patch_slot_number.astype(jnp.int32)
    picked = jnp.take(boundary_energy_current, columns, axis=1)
    source = jnp.sum(jacobian_quad_factors * picked, axis=0)
    layer = source.reshape(N_FLUID, N_SOLID, CX, CY).transpose(0, 2, 1, 3).reshape(SOLID_COUNT_X, SOLID_COUNT_Y)
    forcing_entries = thermal_inertia * earlier_thermal_state
    forcing_entries = forcing_entries.at[:, :, SOLID_COUNT_Z - 1].add(layer)
    diagonal = 6.0 + thermal_inertia
    thermal_state_guess = earlier_thermal_state
    equation_misfit = forcing_entries - matrix_action(thermal_state_guess, thermal_inertia)
    precond = equation_misfit / diagonal
    update_course = precond
    norm_now = jnp.sum(equation_misfit * precond)
    for iteration in range(ITERS):
        image = matrix_action(update_course, thermal_inertia)
        update_multiplier = norm_now / jnp.sum(update_course * image)
        thermal_state_guess = thermal_state_guess + update_multiplier * update_course
        equation_misfit = equation_misfit - update_multiplier * image
        precond = equation_misfit / diagonal
        norm_next = jnp.sum(equation_misfit * precond)
        update_course = precond + (norm_next / norm_now) * update_course
        norm_now = norm_next
    return thermal_state_guess, equation_misfit
```

```python
import functools

import jax
import jax.numpy as jnp
from jax import lax
from jax.experimental import pallas as pl
from jax.experimental.pallas import tpu as pltpu

ITERS = 3
W = 4
YO = 8
MESH = pl.DeviceIdType.MESH


def kernel(
    nf, ns, t_hbm, i_hbm, face_hbm, jac_hbm, own_hbm, slot_hbm,
    x_hbm, r_hbm,
    t_ext, i_ext, dinv, v0, v1, v2, v3, gath, onehot, jac, own, slot,
    pk_lo, pk_hi, rc_lo, rc_hi, src, src_rc, src_t, sums, xo, ro,
    in_sem, h_send, h_recv, f_send, f_recv, f_relay, s_send, s_recv, a_send, a_recv, out_sem,
):
    n = nf * ns
    cx, cy = t_hbm.shape[0], t_hbm.shape[1]
    f, s = lax.axis_index("fluid"), lax.axis_index("solid")
    me = f * ns + s
    up_f, dn_f = lax.rem(f + 1, nf), lax.rem(f + nf - 1, nf)
    up_s, dn_s = lax.rem(s + 1, ns), lax.rem(s + ns - 1, ns)
    lx = pl.ds(W, cx)
    ly = pl.ds(YO, cy)

    loads = [
        pltpu.make_async_copy(face_hbm, gath.at[f], in_sem.at[0]),
        pltpu.make_async_copy(t_hbm, t_ext.at[lx, ly], in_sem.at[1]),
        pltpu.make_async_copy(i_hbm, i_ext.at[lx, ly], in_sem.at[2]),
        pltpu.make_async_copy(slot_hbm, slot, in_sem.at[3]),
        pltpu.make_async_copy(own_hbm, own, in_sem.at[4]),
        pltpu.make_async_copy(jac_hbm, jac, in_sem.at[5]),
    ]
    for load in loads:
        load.start()

    barrier = pltpu.get_barrier_semaphore()

    def greet(k, _):
        to = lax.rem(me + k, n)
        pl.semaphore_signal(
            barrier, inc=1, device_id={"fluid": to // ns, "solid": lax.rem(to, ns)}, device_id_type=MESH
        )
        return 0

    lax.fori_loop(1, n, greet, 0)

    loads[1].wait()
    loads[2].wait()
    pk_lo[:, 0:W, :] = t_ext[lx, YO:YO + W, :]
    pk_lo[:, W:2 * W, :] = i_ext[lx, YO:YO + W, :]
    pk_hi[:, 0:W, :] = t_ext[lx, YO + cy - W:YO + cy, :]
    pk_hi[:, W:2 * W, :] = i_ext[lx, YO + cy - W:YO + cy, :]
    loads[0].wait()
    pl.semaphore_wait(barrier, n - 1)

    def remote(a, b, send, recv, to_f, to_s):
        return pltpu.make_async_remote_copy(
            src_ref=a, dst_ref=b, send_sem=send, recv_sem=recv,
            device_id={"fluid": to_f, "solid": to_s}, device_id_type=MESH,
        )

    pairs = nf // 2
    side = lax.rem(f, 2)
    mate = f + 1 - 2 * side
    mine = f // 2

    def face_copy(to_f, block, send):
        return remote(gath.at[block], gath.at[block], send, f_recv.at[block], to_f, s)

    def peer(j):
        return 2 * lax.rem(mine + j, pairs) + side

    def back(j):
        return 2 * lax.rem(mine + pairs - j, pairs) + side

    def send_face(j, _):
        to = peer(j)
        face_copy(to, f, f_send.at[to]).start()
        return 0

    lax.fori_loop(1, pairs, send_face, 0)
    face_copy(mate, f, f_send.at[mate]).start()

    hi, lo = pl.ds(W + cx, W), pl.ds(0, W)
    first, last = pl.ds(W, W), pl.ds(cx, W)
    pfirst, plast = pl.ds(0, W), pl.ds(cx - W, W)
    halo = []

    def add(a, b, to_f, to_s):
        k = len(halo)
        halo.append(remote(a, b, h_send.at[k], h_recv.at[k], to_f, to_s))

    add(pk_lo, rc_hi.at[lx], f, dn_s)
    add(pk_hi, rc_lo.at[lx], f, up_s)
    add(t_ext.at[first, ly], t_ext.at[hi, ly], dn_f, s)
    add(t_ext.at[last, ly], t_ext.at[lo, ly], up_f, s)
    add(i_ext.at[first, ly], i_ext.at[hi, ly], dn_f, s)
    add(i_ext.at[last, ly], i_ext.at[lo, ly], up_f, s)
    add(pk_lo.at[pfirst], rc_hi.at[hi], dn_f, dn_s)
    add(pk_lo.at[plast], rc_hi.at[lo], up_f, dn_s)
    add(pk_hi.at[pfirst], rc_lo.at[hi], dn_f, up_s)
    add(pk_hi.at[plast], rc_lo.at[lo], up_f, up_s)
    for copy in halo:
        copy.start()

    loads[3].wait()
    loads[4].wait()
    loads[5].wait()
    faces, rows = onehot.shape
    step = 64

    def make_hot(k, _):
        at = pl.multiple_of(k * step, step)
        ids = lax.broadcasted_iota(jnp.int32, (step, rows), 0) + at
        onehot[pl.ds(at, step), :] = jnp.where(ids == slot[...], 1.0, 0.0).astype(jnp.bfloat16)
        return 0

    lax.fori_loop(0, faces // step, make_hot, 0)

    def pick(block, total):
        g = gath[block]
        high = g.astype(jnp.bfloat16)
        low = (g - high.astype(jnp.float32)).astype(jnp.bfloat16)
        both = jnp.dot(
            jnp.concatenate([high, low], axis=0), onehot[...], preferred_element_type=jnp.float32
        )
        q = g.shape[0]
        part = jnp.sum((both[:q] + both[q:]) * jac[...], axis=0, keepdims=True)
        return jnp.where(own[...] == block, part, total)

    total = pick(f, jnp.zeros((1, rows), jnp.float32))

    for copy in halo:
        copy.wait()

    ext = pl.ds(YO - W, cy + 2 * W)
    lanes = t_ext.shape[2]
    lane = lax.broadcasted_iota(jnp.int32, (1, lanes), 1)

    def beside(ref, x, lo_y, num):
        c = ref[x, pl.ds(lo_y, num), :]
        z = jnp.where(lane == 0, 0.0, pltpu.roll(c, 1, 1))
        z = z + jnp.where(lane == lanes - 1, 0.0, pltpu.roll(c, lanes - 1, 1))
        z = z + (ref[x - 1, pl.ds(lo_y, num), :] + ref[x + 1, pl.ds(lo_y, num), :])
        z = z + (ref[x, pl.ds(lo_y - 1, num), :] + ref[x, pl.ds(lo_y + 1, num), :])
        return c, z

    def inverse(a):
        return 1.0 / (6.0 + a)

    def prep(x, _):
        ok = ((x >= W) | (f > 0)) & ((x < W + cx) | (f < nf - 1))
        ok_lo, ok_hi = ok & (s > 0), ok & (s < ns - 1)
        t_ext[x, ly, :] = jnp.where(ok, t_ext[x, ly, :], 0.0)
        dinv[x, ly, :] = jnp.where(ok, inverse(i_ext[x, ly, :]), 0.0)
        a, b = rc_lo[x], rc_hi[x]
        t_ext[x, YO - W:YO, :] = jnp.where(ok_lo, a[:W], 0.0)
        dinv[x, YO - W:YO, :] = jnp.where(ok_lo, inverse(a[W:]), 0.0)
        t_ext[x, YO + cy:YO + cy + W, :] = jnp.where(ok_hi, b[:W], 0.0)
        dinv[x, YO + cy:YO + cy + W, :] = jnp.where(ok_hi, inverse(b[W:]), 0.0)
        return 0

    lax.fori_loop(0, cx + 2 * W, prep, 0)

    def start_field(x, _):
        c, z = beside(t_ext, x, YO - W, cy + 2 * W)
        v0[x, ext, :] = dinv[x, ext, :] * (z - 6.0 * c)
        return 0

    lax.fori_loop(1, cx + 2 * W - 1, start_field, 0)

    def take(j, total):
        block = back(j)
        face_copy(peer(j), block, f_send.at[peer(j)]).wait_recv()
        face_copy(mate, block, f_relay.at[block]).start()
        return pick(block, total)

    total = lax.fori_loop(1, pairs, take, total)

    def take_mate(j, total):
        block = back(j) + 1 - 2 * side
        face_copy(mate, block, f_send.at[mate]).wait_recv()
        return pick(block, total)

    total = lax.fori_loop(0, pairs, take_mate, total)
    src[...] = total.reshape(src.shape)

    around = [
        (a, b) for a in (-1, 0, 1) for b in (-1, 0, 1) if (a, b) != (0, 0)
    ]
    to_f, to_s = {-1: dn_f, 0: f, 1: up_f}, {-1: dn_s, 0: s, 1: up_s}
    spread = [
        remote(src, src_rc.at[k], s_send.at[k], s_recv.at[k], to_f[-a], to_s[-b])
        for k, (a, b) in enumerate(around)
    ]
    for copy in spread:
        copy.start()

    def turned(tile):
        return jnp.concatenate(
            [tile.T, jnp.zeros((tile.shape[1], lanes - tile.shape[0]), jnp.float32)], axis=1
        )

    src_t[1, 1] = turned(src[...])
    for copy in spread:
        copy.wait_recv()
    for k, (a, b) in enumerate(around):
        src_t[a + 1, b + 1] = turned(src_rc[k])
    per = lanes // cy

    end = lane == lanes - 1

    def add_source(x, _):
        g = x + cx - W
        a = g // cx
        xl = g - a * cx
        col = xl // per
        at = (xl - col * per) * cy

        def column(b, y0, num):
            y = pl.multiple_of(at, cy) + y0
            return jnp.where(end, pltpu.roll(src_t[a, b, pl.ds(y, num), :], lanes - 1 - col, 1), 0.0)

        below, inner, above = column(0, cy - 8, 8), column(1, 0, cy), column(2, 0, 8)
        v0[x, ly, :] = v0[x, ly, :] + dinv[x, ly, :] * inner
        ylo, yhi = pl.ds(YO - W, W), pl.ds(YO + cy, W)
        v0[x, ylo, :] = v0[x, ylo, :] + dinv[x, ylo, :] * below[8 - W:]
        v0[x, yhi, :] = v0[x, yhi, :] + dinv[x, yhi, :] * above[:W]
        return 0

    lax.fori_loop(1, cx + 2 * W - 1, add_source, 0)

    def power(ref, out):
        def one(x, _):
            _, z = beside(ref, x, YO - W, cy + 2 * W)
            out[x, ext, :] = dinv[x, ext, :] * z
            return 0
        return one

    lax.fori_loop(2, cx + 2 * W - 2, power(v0, v1), 0)
    lax.fori_loop(3, cx + 2 * W - 3, power(v1, v2), 0)

    def fold(a):
        return jnp.sum(a.reshape(cy // 8, 8, lanes), axis=0)

    def last_power(x, acc):
        c2, z = beside(v2, x, YO, cy)
        c0, c1 = v0[x, ly, :], v1[x, ly, :]
        d = 6.0 + i_ext[x, ly, :]
        v3[x, ly, :] = dinv[x, ly, :] * z
        d0, d1, d2 = d * c0, d * c1, d * c2
        parts = (c0 * d0, c1 * d0, c1 * d1, c2 * d1, c2 * d2, c2 * z)
        return tuple(a + fold(p) for a, p in zip(acc, parts))

    zero = jnp.zeros((8, lanes), jnp.float32)
    acc = lax.fori_loop(W, W + cx, last_power, (zero,) * 6)
    row = jnp.zeros((1, lanes), jnp.float32)
    for k, a in enumerate(acc):
        whole = jnp.sum(jnp.sum(a, axis=0, keepdims=True), axis=1, keepdims=True)
        row = jnp.where(lane == k, whole, row)
    sums[me] = row

    def sum_copy(k, source):
        to = lax.rem(me + k, n)
        return remote(
            sums.at[source], sums.at[source], a_send.at[k], a_recv.at[source], to // ns, lax.rem(to, ns)
        )

    def send_sum(k, _):
        sum_copy(k, me).start()
        return 0

    lax.fori_loop(1, n, send_sum, 0)

    def await_sum(k, _):
        sum_copy(k, lax.rem(me + k, n)).wait_recv()
        return 0

    lax.fori_loop(1, n, await_sum, 0)
    mean = jnp.sum(sums[...], axis=0)
    mu = [
        jnp.broadcast_to(jnp.sum(jnp.where(lane == k, mean, 0.0), axis=1, keepdims=True), (1, lanes))
        for k in range(6)
    ]

    def inner(a, b):
        out = None
        for i, p in enumerate(a):
            for j, q in enumerate(b):
                term = p * q * mu[i + j]
                out = term if out is None else out + term
        return out

    one = jnp.ones((1, lanes), jnp.float32)
    z, p, c = [one], [one], []
    rz = mu[0]
    for it in range(ITERS):
        w = [p[0]] + [p[i] - p[i - 1] for i in range(1, len(p))] + [-p[-1]]
        alpha = rz / inner(p, w)
        c = [(c[i] if i < len(c) else 0.0) + alpha * p[i] for i in range(len(p))]
        if it + 1 < ITERS:
            z = [(z[i] if i < len(z) else 0.0) - alpha * w[i] for i in range(len(w))]
            new = inner(z, z)
            ratio = new / rz
            p = [z[i] + (ratio * p[i] if i < len(p) else 0.0) for i in range(len(z))]
            rz = new
    e0, e1, e2 = one - c[0], c[0] - c[1], c[1] - c[2]

    chunk = 8
    outs = []
    for base in range(0, cx, chunk):
        def finish(k, _, base=base):
            x = base + k + W
            c0, c1, c2, c3 = v0[x, ly, :], v1[x, ly, :], v2[x, ly, :], v3[x, ly, :]
            xo[base + k] = t_ext[x, ly, :] + (c[0] * c0 + c[1] * c1 + c[2] * c2)
            ro[base + k] = (6.0 + i_ext[x, ly, :]) * (e0 * c0 + e1 * c1 + e2 * c2 + c[2] * c3)
            return 0

        lax.fori_loop(0, chunk, finish, 0)
        part = pl.ds(base, chunk)
        k = base // chunk
        for copy in (
            pltpu.make_async_copy(xo.at[part], x_hbm.at[part], out_sem.at[2 * k]),
            pltpu.make_async_copy(ro.at[part], r_hbm.at[part], out_sem.at[2 * k + 1]),
        ):
            copy.start()
            outs.append(copy)

    for copy in spread:
        copy.wait_send()

    def sent_face(j, _):
        to = peer(j)
        face_copy(to, f, f_send.at[to]).wait_send()
        face_copy(mate, back(j), f_relay.at[back(j)]).wait_send()
        return 0

    lax.fori_loop(1, pairs, sent_face, 0)
    face_copy(mate, f, f_send.at[mate]).wait_send()

    def sent_sum(k, _):
        sum_copy(k, me).wait_send()
        return 0

    lax.fori_loop(1, n, sent_sum, 0)
    for copy in outs:
        copy.wait()


def solution(mesh):
    nf, ns = mesh.shape["fluid"], mesh.shape["solid"]
    n = nf * ns

    def per_device(t, inertia, faces, jac, own, slot):
        cx, cy, cz = t.shape
        q, per = faces.shape
        rows = jac.shape[1]
        own, slot = own.reshape(1, rows), slot.reshape(1, rows)
        f32 = jnp.float32
        ext = pltpu.VMEM((cx + 2 * W, cy + 2 * YO, cz), f32)
        vmem = pltpu.VMEM
        dma = pltpu.SemaphoreType.DMA
        shape = jax.ShapeDtypeStruct(t.shape, f32)
        return tuple(pl.pallas_call(
            functools.partial(kernel, nf, ns),
            out_shape=(shape, shape),
            in_specs=[pl.BlockSpec(memory_space=pl.ANY)] * 6,
            out_specs=(pl.BlockSpec(memory_space=pl.ANY),) * 2,
            scratch_shapes=[ext] * 7 + [
                vmem((nf, q, per), f32),
                vmem((per, rows), jnp.bfloat16),
                vmem((q, rows), f32),
                vmem((1, rows), jnp.int32),
                vmem((1, rows), jnp.int32),
                vmem((cx, 2 * W, cz), f32),
                vmem((cx, 2 * W, cz), f32),
                vmem((cx + 2 * W, 2 * W, cz), f32),
                vmem((cx + 2 * W, 2 * W, cz), f32),
                vmem((rows // cz, cz), f32),
                vmem((8, rows // cz, cz), f32),
                vmem((3, 3, cz, cz), f32),
                vmem((n, 1, cz), f32),
                vmem((cx, cy, cz), f32),
                vmem((cx, cy, cz), f32),
                dma((6,)), dma((10,)), dma((10,)), dma((nf,)), dma((nf,)), dma((nf,)),
                dma((8,)), dma((8,)), dma((n,)), dma((n,)), dma((2 * (cx // 8),)),
            ],
            compiler_params=pltpu.CompilerParams(
                collective_id=0, has_side_effects=True, vmem_limit_bytes=50 * 1024 * 1024
            ),
        )(t, inertia, faces, jac, own, slot))

    P = jax.sharding.PartitionSpec
    both = ("fluid", "solid")
    return jax.shard_map(
        per_device,
        mesh=mesh,
        in_specs=(
            P("fluid", "solid", None),
            P("fluid", "solid", None),
            P(None, both),
            P(None, both),
            P(both, None),
            P(both),
        ),
        out_specs=(P("fluid", "solid", None), P("fluid", "solid", None)),
        check_vma=False,
    )
```

```python
import functools

import jax
import jax.numpy as jnp
from jax import lax
from jax.experimental import pallas as pl
from jax.experimental.pallas import tpu as pltpu

ITERS = 3
W = 4
YO = 8
MESH = pl.DeviceIdType.MESH


def sweep(low, high, body, carry=0, unroll=4):
    steps = (high - low) // unroll

    def block(i, carry):
        for j in range(unroll):
            carry = body(low + i * unroll + j, carry)
        return carry

    carry = lax.fori_loop(0, steps, block, carry)
    for x in range(low + steps * unroll, high):
        carry = body(x, carry)
    return carry


def kernel(
    nf, ns, t_hbm, i_hbm, face_hbm, jac_hbm, own_hbm, slot_hbm,
    x_hbm, r_hbm,
    t_ext, i_ext, dinv, v0, v1, v2, v3, gath, onehot, jac, own, slot,
    pk_lo, pk_hi, rc_lo, rc_hi, src, src_rc, src_t, sums, xo, ro,
    in_sem, h_send, h_recv, f_send, f_recv, f_relay, s_send, s_recv, a_send, a_recv, out_sem,
):
    n = nf * ns
    cx, cy = t_hbm.shape[0], t_hbm.shape[1]
    f, s = lax.axis_index("fluid"), lax.axis_index("solid")
    me = f * ns + s
    up_f, dn_f = lax.rem(f + 1, nf), lax.rem(f + nf - 1, nf)
    up_s, dn_s = lax.rem(s + 1, ns), lax.rem(s + ns - 1, ns)
    lx = pl.ds(W, cx)
    ly = pl.ds(YO, cy)

    loads = [
        pltpu.make_async_copy(face_hbm, gath.at[f], in_sem.at[0]),
        pltpu.make_async_copy(t_hbm, t_ext.at[lx, ly], in_sem.at[1]),
        pltpu.make_async_copy(i_hbm, i_ext.at[lx, ly], in_sem.at[2]),
        pltpu.make_async_copy(slot_hbm, slot, in_sem.at[3]),
        pltpu.make_async_copy(own_hbm, own, in_sem.at[4]),
        pltpu.make_async_copy(jac_hbm, jac, in_sem.at[5]),
    ]
    for load in loads:
        load.start()

    src_rc[...] = jnp.zeros_like(src_rc)
    barrier = pltpu.get_barrier_semaphore()

    def greet(k, _):
        to = lax.rem(me + k, n)
        pl.semaphore_signal(
            barrier, inc=1, device_id={"fluid": to // ns, "solid": lax.rem(to, ns)}, device_id_type=MESH
        )
        return 0

    lax.fori_loop(1, n, greet, 0)

    loads[1].wait()
    loads[2].wait()
    pk_lo[:, 0:W, :] = t_ext[lx, YO:YO + W, :]
    pk_lo[:, W:2 * W, :] = i_ext[lx, YO:YO + W, :]
    pk_hi[:, 0:W, :] = t_ext[lx, YO + cy - W:YO + cy, :]
    pk_hi[:, W:2 * W, :] = i_ext[lx, YO + cy - W:YO + cy, :]
    loads[0].wait()
    pl.semaphore_wait(barrier, n - 1)

    def remote(a, b, send, recv, to_f, to_s):
        return pltpu.make_async_remote_copy(
            src_ref=a, dst_ref=b, send_sem=send, recv_sem=recv,
            device_id={"fluid": to_f, "solid": to_s}, device_id_type=MESH,
        )

    pairs = nf // 2
    side = lax.rem(f, 2)
    mate = f + 1 - 2 * side
    mine = f // 2

    def face_copy(to_f, block, send):
        return remote(gath.at[block], gath.at[block], send, f_recv.at[block], to_f, s)

    def peer(j):
        return 2 * lax.rem(mine + j, pairs) + side

    def back(j):
        return 2 * lax.rem(mine + pairs - j, pairs) + side

    def send_face(j, _):
        to = peer(j)
        face_copy(to, f, f_send.at[to]).start()
        return 0

    hi, lo = pl.ds(W + cx, W), pl.ds(0, W)
    first, last = pl.ds(W, W), pl.ds(cx, W)
    pfirst, plast = pl.ds(0, W), pl.ds(cx - W, W)
    halo = []

    to_f, to_s = {-1: dn_f, 0: f, 1: up_f}, {-1: dn_s, 0: s, 1: up_s}

    def there(a, b):
        x, y = f + a, s + b
        return (x >= 0) & (x < nf) & (y >= 0) & (y < ns)

    def add(a, b, df, ds):
        k = len(halo)
        halo.append((remote(a, b, h_send.at[k], h_recv.at[k], to_f[df], to_s[ds]), df, ds))

    add(t_ext.at[first, ly], t_ext.at[hi, ly], -1, 0)
    add(t_ext.at[last, ly], t_ext.at[lo, ly], 1, 0)
    add(i_ext.at[first, ly], i_ext.at[hi, ly], -1, 0)
    add(i_ext.at[last, ly], i_ext.at[lo, ly], 1, 0)
    add(pk_lo, rc_hi.at[lx], 0, -1)
    add(pk_hi, rc_lo.at[lx], 0, 1)
    add(pk_lo.at[pfirst], rc_hi.at[hi], -1, -1)
    add(pk_lo.at[plast], rc_hi.at[lo], 1, -1)
    add(pk_hi.at[pfirst], rc_lo.at[hi], -1, 1)
    add(pk_hi.at[plast], rc_lo.at[lo], 1, 1)

    def each(copies, act, way):
        for copy, df, ds in copies:
            pl.when(there(way * df, way * ds))(functools.partial(act, copy))

    def start(copy):
        copy.start()

    def sent(copy):
        copy.wait_send()

    def received(copy):
        copy.wait_recv()

    each(halo, start, 1)
    lax.fori_loop(1, pairs, send_face, 0)
    face_copy(mate, f, f_send.at[mate]).start()

    loads[3].wait()
    loads[4].wait()
    loads[5].wait()
    faces, rows = onehot.shape
    step = 64

    def make_hot(k, _):
        at = pl.multiple_of(k * step, step)
        ids = lax.broadcasted_iota(jnp.int32, (step, rows), 0) + at
        onehot[pl.ds(at, step), :] = jnp.where(ids == slot[...], 1.0, 0.0).astype(jnp.bfloat16)
        return 0

    lax.fori_loop(0, faces // step, make_hot, 0)

    def pick(block, total):
        g = gath[block]
        high = g.astype(jnp.bfloat16)
        low = (g - high.astype(jnp.float32)).astype(jnp.bfloat16)
        both = jnp.dot(
            jnp.concatenate([high, low], axis=0), onehot[...], preferred_element_type=jnp.float32
        )
        q = g.shape[0]
        part = jnp.sum((both[:q] + both[q:]) * jac[...], axis=0, keepdims=True)
        return jnp.where(own[...] == block, part, total)

    total = pick(f, jnp.zeros((1, rows), jnp.float32))

    each(halo, received, -1)
    each(halo, sent, 1)

    ext = pl.ds(YO - W, cy + 2 * W)
    lanes = t_ext.shape[2]
    lane = lax.broadcasted_iota(jnp.int32, (1, lanes), 1)

    def beside(ref, x, lo_y, num):
        c = ref[x, pl.ds(lo_y, num), :]
        z = jnp.where(lane == 0, 0.0, pltpu.roll(c, 1, 1))
        z = z + jnp.where(lane == lanes - 1, 0.0, pltpu.roll(c, lanes - 1, 1))
        z = z + (ref[x - 1, pl.ds(lo_y, num), :] + ref[x + 1, pl.ds(lo_y, num), :])
        z = z + (ref[x, pl.ds(lo_y - 1, num), :] + ref[x, pl.ds(lo_y + 1, num), :])
        return c, z

    def inverse(a):
        return 1.0 / (6.0 + a)

    def prep(x, _):
        ok = ((x >= W) | (f > 0)) & ((x < W + cx) | (f < nf - 1))
        ok_lo, ok_hi = ok & (s > 0), ok & (s < ns - 1)
        t_ext[x, ly, :] = jnp.where(ok, t_ext[x, ly, :], 0.0)
        dinv[x, ly, :] = jnp.where(ok, inverse(i_ext[x, ly, :]), 0.0)
        a, b = rc_lo[x], rc_hi[x]
        t_ext[x, YO - W:YO, :] = jnp.where(ok_lo, a[:W], 0.0)
        dinv[x, YO - W:YO, :] = jnp.where(ok_lo, inverse(a[W:]), 0.0)
        t_ext[x, YO + cy:YO + cy + W, :] = jnp.where(ok_hi, b[:W], 0.0)
        dinv[x, YO + cy:YO + cy + W, :] = jnp.where(ok_hi, inverse(b[W:]), 0.0)
        return 0

    sweep(0, cx + 2 * W, prep)

    def start_field(x, _):
        c, z = beside(t_ext, x, YO - W, cy + 2 * W)
        v0[x, ext, :] = dinv[x, ext, :] * (z - 6.0 * c)
        return 0

    sweep(1, cx + 2 * W - 1, start_field)

    def take(j, total):
        block = back(j)
        face_copy(peer(j), block, f_send.at[peer(j)]).wait_recv()
        face_copy(mate, block, f_relay.at[block]).start()
        return pick(block, total)

    total = lax.fori_loop(1, pairs, take, total)

    def take_mate(j, total):
        block = back(j) + 1 - 2 * side
        face_copy(mate, block, f_send.at[mate]).wait_recv()
        return pick(block, total)

    total = lax.fori_loop(0, pairs, take_mate, total)
    src[...] = total.reshape(src.shape)

    around = [
        (a, b) for a in (-1, 0, 1) for b in (-1, 0, 1) if (a, b) != (0, 0)
    ]
    spread = [
        (remote(src, src_rc.at[k], s_send.at[k], s_recv.at[k], to_f[-a], to_s[-b]), -a, -b)
        for k, (a, b) in enumerate(around)
    ]
    each(spread, start, 1)

    def turned(tile):
        return jnp.concatenate(
            [tile.T, jnp.zeros((tile.shape[1], lanes - tile.shape[0]), jnp.float32)], axis=1
        )

    src_t[1, 1] = turned(src[...])
    each(spread, received, -1)
    for k, (a, b) in enumerate(around):
        src_t[a + 1, b + 1] = turned(src_rc[k])
    per = lanes // cy

    end = lane == lanes - 1

    def add_source(x, _):
        g = x + cx - W
        a = g // cx
        xl = g - a * cx
        col = xl // per
        at = (xl - col * per) * cy

        def column(b, y0, num):
            y = pl.multiple_of(at, cy) + y0
            return jnp.where(end, pltpu.roll(src_t[a, b, pl.ds(y, num), :], lanes - 1 - col, 1), 0.0)

        below, inner, above = column(0, cy - 8, 8), column(1, 0, cy), column(2, 0, 8)
        v0[x, ly, :] = v0[x, ly, :] + dinv[x, ly, :] * inner
        ylo, yhi = pl.ds(YO - W, W), pl.ds(YO + cy, W)
        v0[x, ylo, :] = v0[x, ylo, :] + dinv[x, ylo, :] * below[8 - W:]
        v0[x, yhi, :] = v0[x, yhi, :] + dinv[x, yhi, :] * above[:W]
        return 0

    sweep(1, cx + 2 * W - 1, add_source)

    def power(ref, out):
        def one(x, _):
            _, z = beside(ref, x, YO - W, cy + 2 * W)
            out[x, ext, :] = dinv[x, ext, :] * z
            return 0
        return one

    sweep(2, cx + 2 * W - 2, power(v0, v1))
    sweep(3, cx + 2 * W - 3, power(v1, v2))

    def fold(a):
        return jnp.sum(a.reshape(cy // 8, 8, lanes), axis=0)

    def last_power(x, acc):
        c2, z = beside(v2, x, YO, cy)
        c0, c1 = v0[x, ly, :], v1[x, ly, :]
        d = 6.0 + i_ext[x, ly, :]
        v3[x, ly, :] = dinv[x, ly, :] * z
        d0, d1, d2 = d * c0, d * c1, d * c2
        parts = (c0 * d0, c1 * d0, c1 * d1, c2 * d1, c2 * d2, c2 * z)
        return tuple(a + fold(p) for a, p in zip(acc, parts))

    zero = jnp.zeros((8, lanes), jnp.float32)
    acc = sweep(W, W + cx, last_power, (zero,) * 6)
    row = jnp.zeros((1, lanes), jnp.float32)
    for k, a in enumerate(acc):
        whole = jnp.sum(jnp.sum(a, axis=0, keepdims=True), axis=1, keepdims=True)
        row = jnp.where(lane == k, whole, row)
    sums[me] = row

    def sum_copy(k, source):
        to = lax.rem(me + k, n)
        return remote(
            sums.at[source], sums.at[source], a_send.at[k], a_recv.at[source], to // ns, lax.rem(to, ns)
        )

    def send_sum(k, _):
        sum_copy(k, me).start()
        return 0

    lax.fori_loop(1, n, send_sum, 0)

    def await_sum(k, _):
        sum_copy(k, lax.rem(me + k, n)).wait_recv()
        return 0

    lax.fori_loop(1, n, await_sum, 0)
    mean = jnp.sum(sums[...], axis=0)
    mu = [
        jnp.broadcast_to(jnp.sum(jnp.where(lane == k, mean, 0.0), axis=1, keepdims=True), (1, lanes))
        for k in range(6)
    ]

    def inner(a, b):
        out = None
        for i, p in enumerate(a):
            for j, q in enumerate(b):
                term = p * q * mu[i + j]
                out = term if out is None else out + term
        return out

    one = jnp.ones((1, lanes), jnp.float32)
    z, p, c = [one], [one], []
    rz = mu[0]
    for it in range(ITERS):
        w = [p[0]] + [p[i] - p[i - 1] for i in range(1, len(p))] + [-p[-1]]
        alpha = rz / inner(p, w)
        c = [(c[i] if i < len(c) else 0.0) + alpha * p[i] for i in range(len(p))]
        if it + 1 < ITERS:
            z = [(z[i] if i < len(z) else 0.0) - alpha * w[i] for i in range(len(w))]
            new = inner(z, z)
            ratio = new / rz
            p = [z[i] + (ratio * p[i] if i < len(p) else 0.0) for i in range(len(z))]
            rz = new
    e0, e1, e2 = one - c[0], c[0] - c[1], c[1] - c[2]

    chunk = 8
    outs = []
    for base in range(0, cx, chunk):
        def finish(k, _, base=base):
            x = base + k + W
            c0, c1, c2, c3 = v0[x, ly, :], v1[x, ly, :], v2[x, ly, :], v3[x, ly, :]
            xo[base + k] = t_ext[x, ly, :] + (c[0] * c0 + c[1] * c1 + c[2] * c2)
            ro[base + k] = (6.0 + i_ext[x, ly, :]) * (e0 * c0 + e1 * c1 + e2 * c2 + c[2] * c3)
            return 0

        sweep(0, chunk, finish)
        part = pl.ds(base, chunk)
        k = base // chunk
        for copy in (
            pltpu.make_async_copy(xo.at[part], x_hbm.at[part], out_sem.at[2 * k]),
            pltpu.make_async_copy(ro.at[part], r_hbm.at[part], out_sem.at[2 * k + 1]),
        ):
            copy.start()
            outs.append(copy)

    each(spread, sent, 1)

    def sent_face(j, _):
        to = peer(j)
        face_copy(to, f, f_send.at[to]).wait_send()
        face_copy(mate, back(j), f_relay.at[back(j)]).wait_send()
        return 0

    lax.fori_loop(1, pairs, sent_face, 0)
    face_copy(mate, f, f_send.at[mate]).wait_send()

    def sent_sum(k, _):
        sum_copy(k, me).wait_send()
        return 0

    lax.fori_loop(1, n, sent_sum, 0)
    for copy in outs:
        copy.wait()


def solution(mesh):
    nf, ns = mesh.shape["fluid"], mesh.shape["solid"]
    n = nf * ns

    def per_device(t, inertia, faces, jac, own, slot):
        cx, cy, cz = t.shape
        q, per = faces.shape
        rows = jac.shape[1]
        own, slot = own.reshape(1, rows), slot.reshape(1, rows)
        f32 = jnp.float32
        ext = pltpu.VMEM((cx + 2 * W, cy + 2 * YO, cz), f32)
        vmem = pltpu.VMEM
        dma = pltpu.SemaphoreType.DMA
        shape = jax.ShapeDtypeStruct(t.shape, f32)
        return tuple(pl.pallas_call(
            functools.partial(kernel, nf, ns),
            out_shape=(shape, shape),
            in_specs=[pl.BlockSpec(memory_space=pltpu.HBM)] * 6,
            out_specs=(pl.BlockSpec(memory_space=pltpu.HBM),) * 2,
            scratch_shapes=[ext] * 7 + [
                vmem((nf, q, per), f32),
                vmem((per, rows), jnp.bfloat16),
                vmem((q, rows), f32),
                vmem((1, rows), jnp.int32),
                vmem((1, rows), jnp.int32),
                vmem((cx, 2 * W, cz), f32),
                vmem((cx, 2 * W, cz), f32),
                vmem((cx + 2 * W, 2 * W, cz), f32),
                vmem((cx + 2 * W, 2 * W, cz), f32),
                vmem((rows // cz, cz), f32),
                vmem((8, rows // cz, cz), f32),
                vmem((3, 3, cz, cz), f32),
                vmem((n, 1, cz), f32),
                vmem((cx, cy, cz), f32),
                vmem((cx, cy, cz), f32),
                dma((6,)), dma((10,)), dma((10,)), dma((nf,)), dma((nf,)), dma((nf,)),
                dma((8,)), dma((8,)), dma((n,)), dma((n,)), dma((2 * (cx // 8),)),
            ],
            compiler_params=pltpu.CompilerParams(
                collective_id=0, has_side_effects=True, vmem_limit_bytes=63 * 1024 * 1024
            ),
        )(t, inertia, faces, jac, own, slot))

    P = jax.sharding.PartitionSpec
    both = ("fluid", "solid")
    return jax.shard_map(
        per_device,
        mesh=mesh,
        in_specs=(
            P("fluid", "solid", None),
            P("fluid", "solid", None),
            P(None, both),
            P(None, both),
            P(both, None),
            P(both),
        ),
        out_specs=(P("fluid", "solid", None), P("fluid", "solid", None)),
        check_vma=False,
    )
```

```python
import functools

import jax
import jax.numpy as jnp
from jax import lax
from jax.experimental import pallas as pl
from jax.experimental.pallas import tpu as pltpu

ITERS = 3
W = 4
YO = 8
MESH = pl.DeviceIdType.MESH


def sweep(low, high, body, carry=0, unroll=4):
    steps = (high - low) // unroll

    def block(i, carry):
        for j in range(unroll):
            carry = body(low + i * unroll + j, carry)
        return carry

    carry = lax.fori_loop(0, steps, block, carry)
    for x in range(low + steps * unroll, high):
        carry = body(x, carry)
    return carry


def kernel(
    nf, ns, t_hbm, i_hbm, face_hbm, jac_hbm, own_hbm, slot_hbm,
    xo, ro,
    t_ext, i_ext, dinv, v0, v1, v2, v3, gath, onehot, jac, own, slot,
    pk_lo, pk_hi, rc_lo, rc_hi, src, src_rc, src_t, sums,
    in_sem, h_send, h_recv, f_send, f_recv, f_relay, s_send, s_recv, a_send, a_recv,
):
    n = nf * ns
    cx, cy = t_hbm.shape[0], t_hbm.shape[1]
    f, s = lax.axis_index("fluid"), lax.axis_index("solid")
    me = f * ns + s
    up_f, dn_f = lax.rem(f + 1, nf), lax.rem(f + nf - 1, nf)
    up_s, dn_s = lax.rem(s + 1, ns), lax.rem(s + ns - 1, ns)
    lx = pl.ds(W, cx)
    ly = pl.ds(YO, cy)

    loads = [
        pltpu.make_async_copy(face_hbm, gath.at[f], in_sem.at[0]),
        pltpu.make_async_copy(t_hbm, t_ext.at[lx, ly], in_sem.at[1]),
        pltpu.make_async_copy(i_hbm, i_ext.at[lx, ly], in_sem.at[2]),
        pltpu.make_async_copy(slot_hbm, slot, in_sem.at[3]),
        pltpu.make_async_copy(own_hbm, own, in_sem.at[4]),
        pltpu.make_async_copy(jac_hbm, jac, in_sem.at[5]),
    ]
    for load in loads:
        load.start()

    src_rc[...] = jnp.zeros_like(src_rc)
    barrier = pltpu.get_barrier_semaphore()

    turns = [s] + [lax.rem(s + k, ns) for k in range(1, ns)]

    def others(act):
        def line(k, _):
            to = lax.rem(f + k, nf)
            for turn in turns:
                act(to, turn)
            return 0

        for turn in turns[1:]:
            act(f, turn)
        lax.fori_loop(1, nf, line, 0)

    def greet(a, b):
        pl.semaphore_signal(
            barrier, inc=1, device_id={"fluid": a, "solid": b}, device_id_type=MESH
        )

    others(greet)

    loads[0].wait()
    pl.semaphore_wait(barrier, n - 1)

    def remote(a, b, send, recv, to_f, to_s):
        return pltpu.make_async_remote_copy(
            src_ref=a, dst_ref=b, send_sem=send, recv_sem=recv,
            device_id={"fluid": to_f, "solid": to_s}, device_id_type=MESH,
        )

    pairs = nf // 2
    side = lax.rem(f, 2)
    mate = f + 1 - 2 * side
    mine = f // 2

    def face_copy(to_f, block, send):
        return remote(gath.at[block], gath.at[block], send, f_recv.at[block], to_f, s)

    tree = pairs == 4
    if tree:
        across, along = mine + 1 - 2 * lax.rem(mine, 2), lax.rem(mine + 2, 4)
        pair_a = across + side * (along - across)
        pair_b = along + side * (across - along)
        pair_d = lax.rem(across + 2, 4)
        near_a, near_b, far = 2 * pair_a + side, 2 * pair_b + side, 2 * pair_d + side

    def peer(j):
        return 2 * lax.rem(mine + j, pairs) + side

    def back(j):
        return 2 * lax.rem(mine + pairs - j, pairs) + side

    def send_face(j, _):
        to = peer(j)
        face_copy(to, f, f_send.at[to]).start()
        return 0

    hi, lo = pl.ds(W + cx, W), pl.ds(0, W)
    first, last = pl.ds(W, W), pl.ds(cx, W)
    pfirst, plast = pl.ds(0, W), pl.ds(cx - W, W)
    halo = []

    to_f, to_s = {-1: dn_f, 0: f, 1: up_f}, {-1: dn_s, 0: s, 1: up_s}

    def there(a, b):
        x, y = f + a, s + b
        return (x >= 0) & (x < nf) & (y >= 0) & (y < ns)

    def add(a, b, df, ds):
        k = len(halo)
        halo.append((remote(a, b, h_send.at[k], h_recv.at[k], to_f[df], to_s[ds]), df, ds))

    add(t_ext.at[first, ly], t_ext.at[hi, ly], -1, 0)
    add(t_ext.at[last, ly], t_ext.at[lo, ly], 1, 0)
    add(i_ext.at[pl.ds(W, W - 1), ly], i_ext.at[pl.ds(W + cx, W - 1), ly], -1, 0)
    add(i_ext.at[pl.ds(cx + 1, W - 1), ly], i_ext.at[pl.ds(1, W - 1), ly], 1, 0)
    add(pk_lo, rc_hi.at[lx], 0, -1)
    add(pk_hi, rc_lo.at[lx], 0, 1)
    add(pk_lo.at[pfirst], rc_hi.at[hi], -1, -1)
    add(pk_lo.at[plast], rc_hi.at[lo], 1, -1)
    add(pk_hi.at[pfirst], rc_lo.at[hi], -1, 1)
    add(pk_hi.at[plast], rc_lo.at[lo], 1, 1)

    def each(copies, act, way):
        for copy, df, ds in copies:
            pl.when(there(way * df, way * ds))(functools.partial(act, copy))

    def start(copy):
        copy.start()

    def sent(copy):
        copy.wait_send()

    def received(copy):
        copy.wait_recv()

    if tree:
        direct = [face_copy(near_a, f, f_send.at[0]), face_copy(near_b, f, f_send.at[1]), face_copy(mate, f, f_send.at[2])]
        onward = face_copy(near_b, near_a, f_send.at[3])
        passed = [face_copy(mate, block, f_relay.at[k]) for k, block in enumerate((near_a, near_b, far))]
        for copy in direct:
            copy.start()
    else:
        lax.fori_loop(1, pairs, send_face, 0)
        face_copy(mate, f, f_send.at[mate]).start()
    loads[1].wait()
    loads[2].wait()
    pk_lo[:, 0:W, :] = t_ext[lx, YO:YO + W, :]
    pk_lo[:, W:2 * W, :] = i_ext[lx, YO:YO + W, :]
    pk_hi[:, 0:W, :] = t_ext[lx, YO + cy - W:YO + cy, :]
    pk_hi[:, W:2 * W, :] = i_ext[lx, YO + cy - W:YO + cy, :]
    each(halo, start, 1)

    loads[3].wait()
    loads[4].wait()
    loads[5].wait()
    faces, rows = onehot.shape
    step = 64

    def make_hot(k, _):
        at = pl.multiple_of(k * step, step)
        ids = lax.broadcasted_iota(jnp.int32, (step, rows), 0) + at
        onehot[pl.ds(at, step), :] = jnp.where(ids == slot[...], 1.0, 0.0).astype(jnp.bfloat16)
        return 0

    lax.fori_loop(0, faces // step, make_hot, 0)

    def pick(block, total):
        g = gath[block]
        high = g.astype(jnp.bfloat16)
        low = (g - high.astype(jnp.float32)).astype(jnp.bfloat16)
        both = jnp.dot(
            jnp.concatenate([high, low], axis=0), onehot[...], preferred_element_type=jnp.float32
        )
        q = g.shape[0]
        part = jnp.sum((both[:q] + both[q:]) * jac[...], axis=0, keepdims=True)
        return jnp.where(own[...] == block, part, total)

    total = pick(f, jnp.zeros((1, rows), jnp.float32))
    if tree:
        face_copy(mate, mate, f_send.at[0]).wait_recv()
        total = pick(mate, total)
        face_copy(mate, near_a, f_send.at[0]).wait_recv()
        onward.start()
        passed[0].start()
        total = pick(near_a, total)
        face_copy(mate, near_b, f_send.at[0]).wait_recv()
        passed[1].start()
        total = pick(near_b, total)

    each(halo, received, -1)
    each(halo, sent, 1)

    ext = pl.ds(YO - W, cy + 2 * W)
    lanes = t_ext.shape[2]
    lane = lax.broadcasted_iota(jnp.int32, (1, lanes), 1)

    def beside(ref, x, lo_y, num):
        c = ref[x, pl.ds(lo_y, num), :]
        z = jnp.where(lane == 0, 0.0, pltpu.roll(c, 1, 1))
        z = z + jnp.where(lane == lanes - 1, 0.0, pltpu.roll(c, lanes - 1, 1))
        z = z + (ref[x - 1, pl.ds(lo_y, num), :] + ref[x + 1, pl.ds(lo_y, num), :])
        z = z + (ref[x, pl.ds(lo_y - 1, num), :] + ref[x, pl.ds(lo_y + 1, num), :])
        return c, z

    def inverse(a):
        return 1.0 / (6.0 + a)

    def prep(x, _):
        ok = ((x >= W) | (f > 0)) & ((x < W + cx) | (f < nf - 1))
        ok_lo, ok_hi = ok & (s > 0), ok & (s < ns - 1)
        t_ext[x, ly, :] = jnp.where(ok, t_ext[x, ly, :], 0.0)
        dinv[x, ly, :] = jnp.where(ok, inverse(i_ext[x, ly, :]), 0.0)
        a, b = rc_lo[x], rc_hi[x]
        t_ext[x, YO - W:YO, :] = jnp.where(ok_lo, a[:W], 0.0)
        dinv[x, YO - W:YO, :] = jnp.where(ok_lo, inverse(a[W:]), 0.0)
        t_ext[x, YO + cy:YO + cy + W, :] = jnp.where(ok_hi, b[:W], 0.0)
        dinv[x, YO + cy:YO + cy + W, :] = jnp.where(ok_hi, inverse(b[W:]), 0.0)
        return 0

    sweep(0, cx + 2 * W, prep, unroll=8)

    def start_field(x, _):
        c, z = beside(t_ext, x, YO - W, cy + 2 * W)
        v0[x, ext, :] = dinv[x, ext, :] * (z - 6.0 * c)
        return 0

    sweep(1, cx + 2 * W - 1, start_field, unroll=10)

    def take(j, total):
        block = back(j)
        face_copy(peer(j), block, f_send.at[peer(j)]).wait_recv()
        face_copy(mate, block, f_relay.at[block]).start()
        return pick(block, total)

    def arrived(block):
        face_copy(mate, block, f_send.at[0]).wait_recv()

    if not tree:
        total = lax.fori_loop(1, pairs, take, total)
    else:
        arrived(far)
        passed[2].start()

    def take_mate(j, total):
        block = back(j) + 1 - 2 * side
        face_copy(mate, block, f_send.at[mate]).wait_recv()
        return pick(block, total)

    if not tree:
        total = lax.fori_loop(0, pairs, take_mate, total)
    else:
        turn_side = 1 - 2 * side
        for block in (near_a + turn_side, near_b + turn_side):
            arrived(block)
            total = pick(block, total)
        total = pick(far, total)
        arrived(far + turn_side)
        total = pick(far + turn_side, total)
    src[...] = total.reshape(src.shape)

    around = [
        (a, b) for a in (-1, 0, 1) for b in (-1, 0, 1) if (a, b) != (0, 0)
    ]
    spread = [
        (remote(src, src_rc.at[k], s_send.at[k], s_recv.at[k], to_f[-a], to_s[-b]), -a, -b)
        for k, (a, b) in enumerate(around)
    ]
    each(spread, start, 1)

    def turned(tile):
        return jnp.concatenate(
            [tile.T, jnp.zeros((tile.shape[1], lanes - tile.shape[0]), jnp.float32)], axis=1
        )

    src_t[1, 1] = turned(src[...])
    per = lanes // cy
    end = lane == lanes - 1

    def place(x):
        g = x + cx - W
        a = g // cx
        xl = g - a * cx
        col = xl // per
        return a, col, (xl - col * per) * cy

    def column(where, b, y0, num):
        a, col, at = where
        y = pl.multiple_of(at, cy) + y0
        return jnp.where(end, pltpu.roll(src_t[a, b, pl.ds(y, num), :], lanes - 1 - col, 1), 0.0)

    def add_inner(x, _):
        v0[x, ly, :] = v0[x, ly, :] + dinv[x, ly, :] * column(place(x), 1, 0, cy)
        return 0

    def add_sides(x, _):
        where = place(x)
        ylo, yhi = pl.ds(YO - W, W), pl.ds(YO + cy, W)
        v0[x, ylo, :] = v0[x, ylo, :] + dinv[x, ylo, :] * column(where, 0, cy - 8, 8)[8 - W:]
        v0[x, yhi, :] = v0[x, yhi, :] + dinv[x, yhi, :] * column(where, 2, 0, 8)[:W]
        return 0

    sweep(W, W + cx, add_inner, unroll=8)
    each(spread, received, -1)
    for k, (a, b) in enumerate(around):
        src_t[a + 1, b + 1] = turned(src_rc[k])
    sweep(1, W, add_inner, unroll=3)
    sweep(W + cx, 2 * W + cx - 1, add_inner, unroll=3)
    sweep(1, cx + 2 * W - 1, add_sides, unroll=10)

    def power(ref, out):
        def one(x, _):
            _, z = beside(ref, x, YO - W, cy + 2 * W)
            out[x, ext, :] = dinv[x, ext, :] * z
            return 0
        return one

    sweep(2, cx + 2 * W - 2, power(v0, v1), unroll=9)
    sweep(3, cx + 2 * W - 3, power(v1, v2), unroll=9)

    def fold(a):
        return jnp.sum(a.reshape(cy // 8, 8, lanes), axis=0)

    def last_power(x, acc):
        c2, z = beside(v2, x, YO, cy)
        c0, c1 = v0[x, ly, :], v1[x, ly, :]
        d = 6.0 + i_ext[x, ly, :]
        v3[x, ly, :] = dinv[x, ly, :] * z
        d0, d1, d2 = d * c0, d * c1, d * c2
        parts = (c0 * d0, c1 * d0, c1 * d1, c2 * d1, c2 * d2, c2 * z)
        return tuple(a + fold(p) for a, p in zip(acc, parts))

    zero = jnp.zeros((8, lanes), jnp.float32)
    acc = sweep(W, W + cx, last_power, (zero,) * 6, unroll=8)
    row = jnp.zeros((1, lanes), jnp.float32)
    for k, a in enumerate(acc):
        whole = jnp.sum(jnp.sum(a, axis=0, keepdims=True), axis=1, keepdims=True)
        row = jnp.where(lane == k, whole, row)
    sums[me] = row

    def sum_copy(a, b, source):
        return remote(sums.at[source], sums.at[source], a_send.at[a * ns + b], a_recv.at[source], a, b)

    others(lambda a, b: sum_copy(a, b, me).start())
    others(lambda a, b: sum_copy(a, b, a * ns + b).wait_recv())
    mean = jnp.sum(sums[...], axis=0)
    mu = [
        jnp.broadcast_to(jnp.sum(jnp.where(lane == k, mean, 0.0), axis=1, keepdims=True), (1, lanes))
        for k in range(6)
    ]

    def inner(a, b):
        out = None
        for i, p in enumerate(a):
            for j, q in enumerate(b):
                term = p * q * mu[i + j]
                out = term if out is None else out + term
        return out

    one = jnp.ones((1, lanes), jnp.float32)
    z, p, c = [one], [one], []
    rz = mu[0]
    for it in range(ITERS):
        w = [p[0]] + [p[i] - p[i - 1] for i in range(1, len(p))] + [-p[-1]]
        alpha = rz / inner(p, w)
        c = [(c[i] if i < len(c) else 0.0) + alpha * p[i] for i in range(len(p))]
        if it + 1 < ITERS:
            z = [(z[i] if i < len(z) else 0.0) - alpha * w[i] for i in range(len(w))]
            new = inner(z, z)
            ratio = new / rz
            p = [z[i] + (ratio * p[i] if i < len(p) else 0.0) for i in range(len(z))]
            rz = new
    e0, e1, e2 = one - c[0], c[0] - c[1], c[1] - c[2]

    chunk = 8
    for base in range(0, cx, chunk):
        def finish(k, _, base=base):
            x = base + k + W
            c0, c1, c2, c3 = v0[x, ly, :], v1[x, ly, :], v2[x, ly, :], v3[x, ly, :]
            xo[base + k] = t_ext[x, ly, :] + (c[0] * c0 + c[1] * c1 + c[2] * c2)
            ro[base + k] = (6.0 + i_ext[x, ly, :]) * (e0 * c0 + e1 * c1 + e2 * c2 + c[2] * c3)
            return 0

        sweep(0, chunk, finish, unroll=chunk)
    each(spread, sent, 1)

    def sent_face(j, _):
        to = peer(j)
        face_copy(to, f, f_send.at[to]).wait_send()
        face_copy(mate, back(j), f_relay.at[back(j)]).wait_send()
        return 0

    if tree:
        for copy in direct + [onward] + passed:
            copy.wait_send()
    else:
        lax.fori_loop(1, pairs, sent_face, 0)
        face_copy(mate, f, f_send.at[mate]).wait_send()

    others(lambda a, b: sum_copy(a, b, me).wait_send())


def deliver(x, r, x_hbm, r_hbm, sem):
    copies = [
        pltpu.make_async_copy(x, x_hbm, sem.at[0]),
        pltpu.make_async_copy(r, r_hbm, sem.at[1]),
    ]
    for copy in copies:
        copy.start()
    for copy in copies:
        copy.wait()


def solution(mesh):
    nf, ns = mesh.shape["fluid"], mesh.shape["solid"]
    n = nf * ns

    def per_device(t, inertia, faces, jac, own, slot):
        cx, cy, cz = t.shape
        q, per = faces.shape
        rows = jac.shape[1]
        own, slot = own.reshape(1, rows), slot.reshape(1, rows)
        f32 = jnp.float32
        ext = pltpu.VMEM((cx + 2 * W, cy + 2 * YO, cz), f32)
        vmem = pltpu.VMEM
        dma = pltpu.SemaphoreType.DMA
        shape = jax.ShapeDtypeStruct(t.shape, f32)
        held = pl.pallas_call(
            functools.partial(kernel, nf, ns),
            out_shape=(pltpu.VMEM(t.shape, f32), pltpu.VMEM(t.shape, f32)),
            in_specs=[pl.BlockSpec(memory_space=pltpu.HBM)] * 6,
            out_specs=(pl.BlockSpec(memory_space=pltpu.VMEM),) * 2,
            scratch_shapes=[ext] * 7 + [
                vmem((nf, q, per), f32),
                vmem((per, rows), jnp.bfloat16),
                vmem((q, rows), f32),
                vmem((1, rows), jnp.int32),
                vmem((1, rows), jnp.int32),
                vmem((cx, 2 * W, cz), f32),
                vmem((cx, 2 * W, cz), f32),
                vmem((cx + 2 * W, 2 * W, cz), f32),
                vmem((cx + 2 * W, 2 * W, cz), f32),
                vmem((rows // cz, cz), f32),
                vmem((8, rows // cz, cz), f32),
                vmem((3, 3, cz, cz), f32),
                vmem((n, 1, cz), f32),
                dma((6,)), dma((10,)), dma((10,)), dma((nf,)), dma((nf,)), dma((nf,)),
                dma((8,)), dma((8,)), dma((n,)), dma((n,)),
            ],
            compiler_params=pltpu.CompilerParams(
                collective_id=0, has_side_effects=True, vmem_limit_bytes=65800000
            ),
        )(t, inertia, faces, jac, own, slot)
        return tuple(pl.pallas_call(
            deliver,
            out_shape=(shape, shape),
            in_specs=[pl.BlockSpec(memory_space=pltpu.VMEM)] * 2,
            out_specs=(pl.BlockSpec(memory_space=pltpu.HBM),) * 2,
            scratch_shapes=[dma((2,))],
        )(*[pltpu.with_memory_space_constraint(a, pltpu.VMEM) for a in held]))

    P = jax.sharding.PartitionSpec
    both = ("fluid", "solid")
    return jax.shard_map(
        per_device,
        mesh=mesh,
        in_specs=(
            P("fluid", "solid", None),
            P("fluid", "solid", None),
            P(None, both),
            P(None, both),
            P(both, None),
            P(both),
        ),
        out_specs=(P("fluid", "solid", None), P("fluid", "solid", None)),
        check_vma=False,
    )
```

```python
import functools

import jax
import jax.numpy as jnp
from jax import lax
from jax.experimental import pallas as pl
from jax.experimental.pallas import tpu as pltpu

ITERS = 3
W = 4
YO = 8
MESH = pl.DeviceIdType.MESH


def sweep(low, high, body, carry=0, unroll=4):
    steps = (high - low) // unroll

    def block(i, carry):
        for j in range(unroll):
            carry = body(low + i * unroll + j, carry)
        return carry

    carry = lax.fori_loop(0, steps, block, carry)
    for x in range(low + steps * unroll, high):
        carry = body(x, carry)
    return carry


def kernel(
    nf, ns, t_hbm, i_hbm, face_hbm, jac_hbm, own_hbm, slot_hbm,
    xo, ro,
    t_ext, i_ext, dinv, v0, v1, v2, v3, gath, onehot, jac, own, slot,
    pk_lo, pk_hi, rc_lo, rc_hi, src, src_rc, src_t, sums,
    in_sem, h_send, h_recv, f_send, f_recv, f_relay, s_send, s_recv, a_send, a_recv,
):
    n = nf * ns
    cx, cy = t_hbm.shape[0], t_hbm.shape[1]
    f, s = lax.axis_index("fluid"), lax.axis_index("solid")
    me = f * ns + s
    up_f, dn_f = lax.rem(f + 1, nf), lax.rem(f + nf - 1, nf)
    up_s, dn_s = lax.rem(s + 1, ns), lax.rem(s + ns - 1, ns)
    lx = pl.ds(W, cx)
    ly = pl.ds(YO, cy)

    loads = [
        pltpu.make_async_copy(face_hbm, gath.at[f], in_sem.at[0]),
        pltpu.make_async_copy(t_hbm, t_ext.at[lx, ly], in_sem.at[1]),
        pltpu.make_async_copy(i_hbm, i_ext.at[lx, ly], in_sem.at[2]),
        pltpu.make_async_copy(slot_hbm, slot, in_sem.at[3]),
        pltpu.make_async_copy(own_hbm, own, in_sem.at[4]),
        pltpu.make_async_copy(jac_hbm, jac, in_sem.at[5]),
    ]
    for load in loads:
        load.start()

    src_rc[...] = jnp.zeros_like(src_rc)
    barrier = pltpu.get_barrier_semaphore()

    turns = [s] + [lax.rem(s + k, ns) for k in range(1, ns)]

    def others(act):
        def line(k, _):
            to = lax.rem(f + k, nf)
            for turn in turns:
                act(to, turn)
            return 0

        for turn in turns[1:]:
            act(f, turn)
        lax.fori_loop(1, nf, line, 0)

    def greet(a, b):
        pl.semaphore_signal(
            barrier, inc=1, device_id={"fluid": a, "solid": b}, device_id_type=MESH
        )

    others(greet)

    loads[0].wait()
    pl.semaphore_wait(barrier, n - 1)

    def remote(a, b, send, recv, to_f, to_s):
        return pltpu.make_async_remote_copy(
            src_ref=a, dst_ref=b, send_sem=send, recv_sem=recv,
            device_id={"fluid": to_f, "solid": to_s}, device_id_type=MESH,
        )

    pairs = nf // 2
    side = lax.rem(f, 2)
    mate = f + 1 - 2 * side
    mine = f // 2

    def face_copy(to_f, block, send):
        return remote(gath.at[block], gath.at[block], send, f_recv.at[block], to_f, s)

    tree = pairs == 4
    if tree:
        across, along = mine + 1 - 2 * lax.rem(mine, 2), lax.rem(mine + 2, 4)
        pair_a = across + side * (along - across)
        pair_b = along + side * (across - along)
        pair_d = lax.rem(across + 2, 4)
        near_a, near_b, far = 2 * pair_a + side, 2 * pair_b + side, 2 * pair_d + side

    def peer(j):
        return 2 * lax.rem(mine + j, pairs) + side

    def back(j):
        return 2 * lax.rem(mine + pairs - j, pairs) + side

    def send_face(j, _):
        to = peer(j)
        face_copy(to, f, f_send.at[to]).start()
        return 0

    hi, lo = pl.ds(W + cx, W), pl.ds(0, W)
    first, last = pl.ds(W, W), pl.ds(cx, W)
    pfirst, plast = pl.ds(0, W - 1), pl.ds(cx - W + 1, W - 1)
    chi, clo = pl.ds(W + cx, W - 1), pl.ds(1, W - 1)
    halo = []

    to_f, to_s = {-1: dn_f, 0: f, 1: up_f}, {-1: dn_s, 0: s, 1: up_s}

    def there(a, b):
        x, y = f + a, s + b
        return (x >= 0) & (x < nf) & (y >= 0) & (y < ns)

    def add(a, b, df, ds):
        k = len(halo)
        halo.append((remote(a, b, h_send.at[k], h_recv.at[k], to_f[df], to_s[ds]), df, ds))

    add(t_ext.at[first, ly], t_ext.at[hi, ly], -1, 0)
    add(t_ext.at[last, ly], t_ext.at[lo, ly], 1, 0)
    add(i_ext.at[pl.ds(W, W - 1), ly], i_ext.at[pl.ds(W + cx, W - 1), ly], -1, 0)
    add(i_ext.at[pl.ds(cx + 1, W - 1), ly], i_ext.at[pl.ds(1, W - 1), ly], 1, 0)
    add(pk_lo, rc_hi.at[lx], 0, -1)
    add(pk_hi, rc_lo.at[lx], 0, 1)
    add(pk_lo.at[pfirst], rc_hi.at[chi], -1, -1)
    add(pk_lo.at[plast], rc_hi.at[clo], 1, -1)
    add(pk_hi.at[pfirst], rc_lo.at[chi], -1, 1)
    add(pk_hi.at[plast], rc_lo.at[clo], 1, 1)

    def each(copies, act, way):
        for copy, df, ds in copies:
            pl.when(there(way * df, way * ds))(functools.partial(act, copy))

    def start(copy):
        copy.start()

    def sent(copy):
        copy.wait_send()

    def received(copy):
        copy.wait_recv()

    if tree:
        direct = [face_copy(near_a, f, f_send.at[0]), face_copy(near_b, f, f_send.at[1]), face_copy(mate, f, f_send.at[2])]
        onward = face_copy(near_b, near_a, f_send.at[3])
        passed = [face_copy(mate, block, f_relay.at[k]) for k, block in enumerate((near_a, near_b, far))]
        for copy in direct:
            copy.start()
    else:
        lax.fori_loop(1, pairs, send_face, 0)
        face_copy(mate, f, f_send.at[mate]).start()
    loads[1].wait()
    loads[2].wait()
    pk_lo[:, 0:W, :] = t_ext[lx, YO:YO + W, :]
    pk_lo[:, W:2 * W, :] = i_ext[lx, YO:YO + W, :]
    pk_hi[:, 0:W, :] = t_ext[lx, YO + cy - W:YO + cy, :]
    pk_hi[:, W:2 * W, :] = i_ext[lx, YO + cy - W:YO + cy, :]
    each(halo, start, 1)

    loads[3].wait()
    loads[4].wait()
    loads[5].wait()
    faces, rows = onehot.shape
    step = 64

    def make_hot(k, _):
        at = pl.multiple_of(k * step, step)
        ids = lax.broadcasted_iota(jnp.int32, (step, rows), 0) + at
        onehot[pl.ds(at, step), :] = jnp.where(ids == slot[...], 1.0, 0.0).astype(jnp.bfloat16)
        return 0

    lax.fori_loop(0, faces // step, make_hot, 0)

    q = jac.shape[0]

    def pick(block, total, *more):
        blocks = (block,) + more
        parts = []
        for one in blocks:
            g = gath[one]
            high = g.astype(jnp.bfloat16)
            parts += [high, (g - high.astype(jnp.float32)).astype(jnp.bfloat16)]
        found = jnp.dot(
            jnp.concatenate(parts, axis=0), onehot[...], preferred_element_type=jnp.float32
        )
        for k, one in enumerate(blocks):
            both = found[2 * q * k:2 * q * (k + 1)]
            part = jnp.sum((both[:q] + both[q:]) * jac[...], axis=0, keepdims=True)
            total = jnp.where(own[...] == one, part, total)
        return total

    total = pick(f, jnp.zeros((1, rows), jnp.float32))
    if tree:
        face_copy(mate, mate, f_send.at[0]).wait_recv()
        total = pick(mate, total)
        face_copy(mate, near_a, f_send.at[0]).wait_recv()
        onward.start()
        passed[0].start()
        total = pick(near_a, total)
        face_copy(mate, near_b, f_send.at[0]).wait_recv()
        passed[1].start()
        total = pick(near_b, total)

    each(halo, received, -1)
    each(halo, sent, 1)

    ext = pl.ds(YO - W, cy + 2 * W)
    lanes = t_ext.shape[2]
    lane = lax.broadcasted_iota(jnp.int32, (1, lanes), 1)

    def beside(ref, x, lo_y, num):
        c = ref[x, pl.ds(lo_y, num), :]
        z = jnp.where(lane == 0, 0.0, pltpu.roll(c, 1, 1))
        z = z + jnp.where(lane == lanes - 1, 0.0, pltpu.roll(c, lanes - 1, 1))
        z = z + (ref[x - 1, pl.ds(lo_y, num), :] + ref[x + 1, pl.ds(lo_y, num), :])
        z = z + (ref[x, pl.ds(lo_y - 1, num), :] + ref[x, pl.ds(lo_y + 1, num), :])
        return c, z

    def inverse(a):
        return 1.0 / (6.0 + a)

    def prep(x, _):
        ok = ((x >= W) | (f > 0)) & ((x < W + cx) | (f < nf - 1))
        ok_lo, ok_hi = ok & (s > 0), ok & (s < ns - 1)
        t_ext[x, ly, :] = jnp.where(ok, t_ext[x, ly, :], 0.0)
        dinv[x, ly, :] = jnp.where(ok, inverse(i_ext[x, ly, :]), 0.0)
        a, b = rc_lo[x], rc_hi[x]
        t_ext[x, YO - W:YO, :] = jnp.where(ok_lo, a[:W], 0.0)
        dinv[x, YO - W:YO, :] = jnp.where(ok_lo, inverse(a[W:]), 0.0)
        t_ext[x, YO + cy:YO + cy + W, :] = jnp.where(ok_hi, b[:W], 0.0)
        dinv[x, YO + cy:YO + cy + W, :] = jnp.where(ok_hi, inverse(b[W:]), 0.0)
        return 0

    sweep(0, cx + 2 * W, prep, unroll=20)

    def start_field(x, _):
        c, z = beside(t_ext, x, YO - W, cy + 2 * W)
        v0[x, ext, :] = dinv[x, ext, :] * (z - 6.0 * c)
        return 0

    sweep(1, cx + 2 * W - 1, start_field, unroll=38)

    def take(j, total):
        block = back(j)
        face_copy(peer(j), block, f_send.at[peer(j)]).wait_recv()
        face_copy(mate, block, f_relay.at[block]).start()
        return pick(block, total)

    def arrived(block):
        face_copy(mate, block, f_send.at[0]).wait_recv()

    if not tree:
        total = lax.fori_loop(1, pairs, take, total)
    else:
        arrived(far)
        passed[2].start()

    def take_mate(j, total):
        block = back(j) + 1 - 2 * side
        face_copy(mate, block, f_send.at[mate]).wait_recv()
        return pick(block, total)

    if not tree:
        total = lax.fori_loop(0, pairs, take_mate, total)
    else:
        turn_side = 1 - 2 * side
        arrived(near_a + turn_side)
        arrived(near_b + turn_side)
        total = pick(near_a + turn_side, total, near_b + turn_side)
        total = pick(far, total)
        arrived(far + turn_side)
        total = pick(far + turn_side, total)
    src[...] = total.reshape(src.shape)

    around = [
        (a, b) for a in (-1, 0, 1) for b in (-1, 0, 1) if (a, b) != (0, 0)
    ]
    spread = [
        (remote(src, src_rc.at[k], s_send.at[k], s_recv.at[k], to_f[-a], to_s[-b]), -a, -b)
        for k, (a, b) in enumerate(around)
    ]
    each(spread, start, 1)

    def turned(tile):
        return jnp.concatenate(
            [tile.T, jnp.zeros((tile.shape[1], lanes - tile.shape[0]), jnp.float32)], axis=1
        )

    src_t[1, 1] = turned(src[...])
    per = lanes // cy
    end = lane == lanes - 1

    def place(x):
        g = x + cx - W
        a = g // cx
        xl = g - a * cx
        col = xl // per
        return a, col, (xl - col * per) * cy

    def column(where, b, y0, num):
        a, col, at = where
        y = at + y0 if isinstance(at, int) else pl.multiple_of(at, cy) + y0
        return jnp.where(end, pltpu.roll(src_t[a, b, pl.ds(y, num), :], lanes - 1 - col, 1), 0.0)

    def add_inner(x, _):
        v0[x, ly, :] = v0[x, ly, :] + dinv[x, ly, :] * column(place(x), 1, 0, cy)
        return 0

    def add_sides(x, _):
        where = place(x)
        ylo, yhi = pl.ds(YO - W, W), pl.ds(YO + cy, W)
        v0[x, ylo, :] = v0[x, ylo, :] + dinv[x, ylo, :] * column(where, 0, cy - 8, 8)[8 - W:]
        v0[x, yhi, :] = v0[x, yhi, :] + dinv[x, yhi, :] * column(where, 2, 0, 8)[:W]
        return 0

    sweep(W, W + cx, add_inner, unroll=32)
    each(spread, received, -1)
    for k, (a, b) in enumerate(around):
        src_t[a + 1, b + 1] = turned(src_rc[k])
    for x in range(1, cx + 2 * W - 1):
        if not W <= x < W + cx:
            add_inner(x, 0)
        add_sides(x, 0)

    def power(ref, out):
        def one(x, _):
            _, z = beside(ref, x, YO - W, cy + 2 * W)
            out[x, ext, :] = dinv[x, ext, :] * z
            return 0
        return one

    sweep(2, cx + 2 * W - 2, power(v0, v1), unroll=36)
    sweep(3, cx + 2 * W - 3, power(v1, v2), unroll=34)

    def fold(a):
        return jnp.sum(a.reshape(cy // 8, 8, lanes), axis=0)

    def last_power(x, acc):
        c2, z = beside(v2, x, YO, cy)
        c0, c1 = v0[x, ly, :], v1[x, ly, :]
        d = 6.0 + i_ext[x, ly, :]
        v3[x, ly, :] = dinv[x, ly, :] * z
        d0, d1, d2 = d * c0, d * c1, d * c2
        parts = (c0 * d0, c1 * d0, c1 * d1, c2 * d1, c2 * d2, c2 * z)
        return tuple(a + fold(p) for a, p in zip(acc, parts))

    zero = jnp.zeros((8, lanes), jnp.float32)
    acc = sweep(W, W + cx, last_power, (zero,) * 6, unroll=32)
    row = jnp.zeros((1, lanes), jnp.float32)
    for k, a in enumerate(acc):
        whole = jnp.sum(jnp.sum(a, axis=0, keepdims=True), axis=1, keepdims=True)
        row = jnp.where(lane == k, whole, row)
    sums[me] = row

    def sum_copy(a, b, source):
        return remote(sums.at[source], sums.at[source], a_send.at[a * ns + b], a_recv.at[source], a, b)

    others(lambda a, b: sum_copy(a, b, me).start())
    each(spread, sent, 1)

    def sent_face(j, _):
        to = peer(j)
        face_copy(to, f, f_send.at[to]).wait_send()
        face_copy(mate, back(j), f_relay.at[back(j)]).wait_send()
        return 0

    if tree:
        for copy in direct + [onward] + passed:
            copy.wait_send()
    else:
        lax.fori_loop(1, pairs, sent_face, 0)
        face_copy(mate, f, f_send.at[mate]).wait_send()

    others(lambda a, b: sum_copy(a, b, a * ns + b).wait_recv())
    mean = jnp.sum(sums[...], axis=0)
    mu = [
        jnp.broadcast_to(jnp.sum(jnp.where(lane == k, mean, 0.0), axis=1, keepdims=True), (1, lanes))
        for k in range(6)
    ]

    def inner(a, b):
        out = None
        for i, p in enumerate(a):
            for j, q in enumerate(b):
                term = p * q * mu[i + j]
                out = term if out is None else out + term
        return out

    one = jnp.ones((1, lanes), jnp.float32)
    z, p, c = [one], [one], []
    rz = mu[0]
    for it in range(ITERS):
        w = [p[0]] + [p[i] - p[i - 1] for i in range(1, len(p))] + [-p[-1]]
        alpha = rz / inner(p, w)
        c = [(c[i] if i < len(c) else 0.0) + alpha * p[i] for i in range(len(p))]
        if it + 1 < ITERS:
            z = [(z[i] if i < len(z) else 0.0) - alpha * w[i] for i in range(len(w))]
            new = inner(z, z)
            ratio = new / rz
            p = [z[i] + (ratio * p[i] if i < len(p) else 0.0) for i in range(len(z))]
            rz = new
    e0, e1, e2 = one - c[0], c[0] - c[1], c[1] - c[2]

    chunk = 8
    for base in range(0, cx, chunk):
        def finish(k, _, base=base):
            x = base + k + W
            c0, c1, c2, c3 = v0[x, ly, :], v1[x, ly, :], v2[x, ly, :], v3[x, ly, :]
            xo[base + k] = t_ext[x, ly, :] + (c[0] * c0 + c[1] * c1 + c[2] * c2)
            ro[base + k] = (6.0 + i_ext[x, ly, :]) * (e0 * c0 + e1 * c1 + e2 * c2 + c[2] * c3)
            return 0

        sweep(0, chunk, finish, unroll=chunk)
    others(lambda a, b: sum_copy(a, b, me).wait_send())


def deliver(x, r, x_hbm, r_hbm, sem):
    copies = [
        pltpu.make_async_copy(x, x_hbm, sem.at[0]),
        pltpu.make_async_copy(r, r_hbm, sem.at[1]),
    ]
    for copy in copies:
        copy.start()
    for copy in copies:
        copy.wait()


def solution(mesh):
    nf, ns = mesh.shape["fluid"], mesh.shape["solid"]
    n = nf * ns

    def per_device(t, inertia, faces, jac, own, slot):
        cx, cy, cz = t.shape
        q, per = faces.shape
        rows = jac.shape[1]
        own, slot = own.reshape(1, rows), slot.reshape(1, rows)
        f32 = jnp.float32
        ext = pltpu.VMEM((cx + 2 * W, cy + 2 * YO, cz), f32)
        vmem = pltpu.VMEM
        dma = pltpu.SemaphoreType.DMA
        shape = jax.ShapeDtypeStruct(t.shape, f32)
        held = pl.pallas_call(
            functools.partial(kernel, nf, ns),
            out_shape=(pltpu.VMEM(t.shape, f32), pltpu.VMEM(t.shape, f32)),
            in_specs=[pl.BlockSpec(memory_space=pltpu.HBM)] * 6,
            out_specs=(pl.BlockSpec(memory_space=pltpu.VMEM),) * 2,
            scratch_shapes=[ext] * 7 + [
                vmem((nf, q, per), f32),
                vmem((per, rows), jnp.bfloat16),
                vmem((q, rows), f32),
                vmem((1, rows), jnp.int32),
                vmem((1, rows), jnp.int32),
                vmem((cx, 2 * W, cz), f32),
                vmem((cx, 2 * W, cz), f32),
                vmem((cx + 2 * W, 2 * W, cz), f32),
                vmem((cx + 2 * W, 2 * W, cz), f32),
                vmem((rows // cz, cz), f32),
                vmem((8, rows // cz, cz), f32),
                vmem((3, 3, cz, cz), f32),
                vmem((n, 1, cz), f32),
                dma((6,)), dma((10,)), dma((10,)), dma((nf,)), dma((nf,)), dma((nf,)),
                dma((8,)), dma((8,)), dma((n,)), dma((n,)),
            ],
            compiler_params=pltpu.CompilerParams(
                collective_id=0, has_side_effects=True, vmem_limit_bytes=65800000
            ),
        )(t, inertia, faces, jac, own, slot)
        return tuple(pl.pallas_call(
            deliver,
            out_shape=(shape, shape),
            in_specs=[pl.BlockSpec(memory_space=pltpu.VMEM)] * 2,
            out_specs=(pl.BlockSpec(memory_space=pltpu.HBM),) * 2,
            scratch_shapes=[dma((2,))],
        )(*[pltpu.with_memory_space_constraint(a, pltpu.VMEM) for a in held]))

    P = jax.sharding.PartitionSpec
    both = ("fluid", "solid")
    return jax.shard_map(
        per_device,
        mesh=mesh,
        in_specs=(
            P("fluid", "solid", None),
            P("fluid", "solid", None),
            P(None, both),
            P(None, both),
            P(both, None),
            P(both),
        ),
        out_specs=(P("fluid", "solid", None), P("fluid", "solid", None)),
        check_vma=False,
    )
```
